512 devices in a mesh: group: 2 (over y), seq: 128 (over x, z), head: 2 (over core).
Axes of the slice: x: 4, y: 2, z: 32, core: 2. Of those that a mesh axis runs over, the one named last changes fastest.
The devices are a block of a 4x8x32 slice.
Arguments:
- queries: bfloat16 [32768, 3, 2560], P(('group', 'seq'), None, 'head'), parts along dimension 0, may hold values from -6 to 6, as said below
- keys: bfloat16 [32768, 512], P(('group', 'seq'), 'head'), parts along dimension 0, may hold values from -6 to 6, as said below
- values: bfloat16 [32768, 512], P(('group', 'seq'), 'head'), parts along dimension 0, may hold values from -6 to 6
- lengths: int32 [128], P('group'), parts along dimension 0, may hold values from 1 to 1024, 16384 in all
- page_owner: int32 [8192, 4], P(('group', 'seq'), 'head'), parts along dimension 0, may hold values from 0 to 127, as said below
- page_slot: int32 [8192, 4], P(('group', 'seq'), 'head'), parts along dimension 0, may hold values from 0 to 63, as said below
Outputs:
- attended: bfloat16 [32768, 3, 2560], P(('group', 'seq'), None, 'head'), parts along dimension 0
- cache_pages: bfloat16 [32768, 4, 256], P(('group', 'seq', 'head')), parts along dimension 0
The draws below stay inside these ranges and needn't reach their ends.
There are 2 independent parts, one for each index of `group`. The reference program is written for one: setup_inputs(seed, part) draws one part's arguments, and reference() takes and returns one part's arrays. A program takes and returns all parts, laid end to end along the dimension named above; each array names one. Nothing has to cross between parts.
Inputs may be any that keep to these rules, and one draw needn't show every extreme that they name: `page_owner`: for each index g of the head axis, the pages of KV heads g * 2 to g * 2 + 1 held by one index of seq include at most one page for any one owner, and that bound is reached; every owner receives exactly 64 such pages. `page_slot`: the pages that one owner receives for one index of the head axis have distinct slots. `queries`: entries lie within the range; they are of order one. `keys`: entries lie within the range; they are of order one. `lengths`: sum to 16384; the largest is exactly 1024.
All inputs are finite; a program needn't handle non-finite values.
Results may differ from the reference program's by a relative error of at most 0.0029.
Values may be sent and summed in bfloat16 or wider, within the bound.
No kernel may reach another device: no remote copies, remote signals or barrier semaphores. Data moves between devices by JAX's collectives and lax.ppermute only.
A program may use at most 64 MiB of HBM per device.

```python
import math
import jax
import jax.numpy as jnp
import numpy as np
from jax import lax

TOK_DEV = 128
LAYERS = 3
KV_HEADS = 4
QPER = 5
HD = 128
PAGE = 4
Q_HEADS = 20
MAXLEN = 1024
REQS = 64
TOKENS = 16384
PAGES = 4096
PAGES_DEV = 32
KV_LOCAL = 2
SLOTS = 64
N_SEQ = 128
N_HEAD = 2


def draw_keys(key, part):
    shape = (TOKENS, KV_HEADS * HD)
    drawn = 1.4 * jax.random.normal(jax.random.fold_in(key, 3), shape, jnp.float32)
    return jnp.clip(drawn, -6.0, 6.0).astype(jnp.bfloat16)


def draw_queries(key, part):
    shape = (TOKENS, LAYERS, Q_HEADS * HD)
    drawn = 1.4 * jax.random.normal(jax.random.fold_in(key, 5), shape, jnp.float32)
    return jnp.clip(drawn, -6.0, 6.0).astype(jnp.bfloat16)


def page_plan(key):
    base = jax.random.fold_in(key, 4242)
    owners = []
    slots = []
    for group in range(N_HEAD):
        group_key = jax.random.fold_in(base, group)
        sigma = jax.random.permutation(jax.random.fold_in(group_key, 1), N_SEQ).astype(jnp.int32)
        tau = jax.random.permutation(jax.random.fold_in(group_key, 2), N_SEQ).astype(jnp.int32)
        offsets = jax.random.permutation(jax.random.fold_in(group_key, 3), max(SLOTS, N_SEQ))[:SLOTS].astype(jnp.int32) % N_SEQ
        row_keys = jax.random.split(jax.random.fold_in(group_key, 4), N_SEQ)
        orders = jax.vmap(lambda subkey: jax.random.permutation(subkey, SLOTS))(row_keys).astype(jnp.int32)
        pages = jnp.arange(PAGES, dtype=jnp.int32)
        source = pages // PAGES_DEV
        within = pages % PAGES_DEV
        local = jnp.arange(KV_LOCAL, dtype=jnp.int32)
        number = within[:, None] * KV_LOCAL + local[None, :]
        owner = sigma[(tau[source][:, None] + offsets[number]) % N_SEQ]
        owners.append(owner)
        slots.append(orders[owner, number])
    return (jnp.concatenate(owners, axis=1).astype(jnp.int32), jnp.concatenate(slots, axis=1).astype(jnp.int32))


def draw_page_owner(key, part):
    return page_plan(key)[0]


def draw_page_slot(key, part):
    return page_plan(key)[1]


def shard_levels(own_key, extent, cuts, smallest, high):
    level = 1.0
    for position, blocks in cuts:
        steps = jax.random.uniform(jax.random.fold_in(jax.random.fold_in(own_key, 6), position), (blocks,), jnp.float32, smallest / len(cuts), high / len(cuts))
        level = level * jnp.repeat(jnp.exp(steps), extent[position] // blocks).reshape((-1,) + (1,) * (len(extent) - 1 - position))
    return level


def split_up(number_of, total, reach, slope):
    portions = [(1 << 20) // math.isqrt(grade ** slope) + 1 for grade in range(2, number_of + 1)]
    rest, counts = total - reach - (number_of - 1), [1] * (number_of - 1)
    while rest > 0:
        movable = [i for i in range(number_of - 1) if counts[i] < reach]
        whole, left = sum([portions[i] for i in movable]), rest
        for i in movable:
            addition = min(reach - counts[i], max(1, left * portions[i] // whole), rest)
            counts[i] = counts[i] + addition
            rest = rest - addition
    return np.array([reach] + counts)


def uneven_parts(key, amount, total, most, lean):
    if amount == 2:
        one = jax.random.randint(key, (), max(1, total - most), min(most, total - 1) + 1)
        return jnp.stack([one, total - one])
    sizes = jnp.asarray(split_up(amount, total, most, lean), jnp.int32)
    couples = (amount - 1) // 2
    donor, receiver = sizes[1:1 + 2 * couples:2], sizes[2:2 + 2 * couples:2]
    margin = jnp.minimum(donor - 1, most - receiver)
    shifted = jax.random.randint(jax.random.fold_in(key, 1), (couples,), 0, 1 << 20) % (margin + 1)
    sizes = sizes.at[1:1 + 2 * couples:2].set(donor - shifted).at[2:2 + 2 * couples:2].set(receiver + shifted)
    return sizes[jax.random.permutation(jax.random.fold_in(key, 2), amount)]


def gaussian(own_key, extent, scale, limit, shards=(), kind=jnp.bfloat16):
    entries = jax.random.normal(own_key, extent, jnp.float32) * scale
    if len(shards) > 0:
        entries = shard_levels(own_key, extent, shards, -0.22, 0.18) * entries
    return jnp.clip(entries, min=-limit, max=limit).astype(kind)


def setup_inputs(seed: int = 0, part: int = 0) -> dict:
    splits = jax.random.split(jax.random.key(seed), 7)
    own_keys = jax.random.split(jax.random.fold_in(splits[6], part), 7)
    return {
        "queries": draw_queries(jax.random.fold_in(jax.random.fold_in(splits[6], part), 71), part),
        "keys": draw_keys(jax.random.fold_in(jax.random.fold_in(splits[6], part), 71), part),
        "values": gaussian(own_keys[2], (TOKENS, KV_HEADS * HD), 1.0, 6.0, ((0, 128), (1, 2))),
        "lengths": uneven_parts(own_keys[3], REQS, TOKENS, MAXLEN, 2).astype(jnp.int32),
        "page_owner": draw_page_owner(jax.random.fold_in(jax.random.fold_in(splits[6], part), 71), part),
        "page_slot": draw_page_slot(jax.random.fold_in(jax.random.fold_in(splits[6], part), 71), part),
    }


def reference(queries, keys, values, lengths, page_owner, page_slot):
    starts = jnp.cumsum(lengths) - lengths
    positions = jnp.arange(TOKENS, dtype=jnp.int32)
    requests = lax.optimization_barrier(jnp.sum((starts[None, :] <= positions[:, None]).astype(jnp.int32), axis=1)) - 1
    lead = MAXLEN
    width = lead + TOK_DEV
    keys_pad = jnp.concatenate([jnp.zeros((lead, KV_HEADS * HD), keys.dtype), keys], axis=0)
    vals_pad = jnp.concatenate([jnp.zeros((lead, KV_HEADS * HD), values.dtype), values], axis=0)
    req_pad = jnp.concatenate([jnp.full((lead,), -1, jnp.int32), requests.astype(jnp.int32)], axis=0)
    scale = 1.0 / math.sqrt(HD)

    def one_block(index):
        begin = (index * TOK_DEV).astype(jnp.int32)
        query_block = lax.dynamic_slice_in_dim(queries, begin, TOK_DEV, 0).astype(jnp.float32)
        query_block = query_block.reshape(TOK_DEV, LAYERS, KV_HEADS, QPER, HD)
        key_block = lax.dynamic_slice_in_dim(keys_pad, begin, width, 0).astype(jnp.float32).reshape(width, KV_HEADS, HD)
        val_block = lax.dynamic_slice_in_dim(vals_pad, begin, width, 0).astype(jnp.float32).reshape(width, KV_HEADS, HD)
        query_pos = begin + jnp.arange(TOK_DEV, dtype=jnp.int32)
        key_pos = begin - lead + jnp.arange(width, dtype=jnp.int32)
        query_req = lax.dynamic_slice_in_dim(requests.astype(jnp.int32), begin, TOK_DEV, 0)
        key_req = lax.dynamic_slice_in_dim(req_pad, begin, width, 0)
        allowed = (query_req[:, None] == key_req[None, :]) & (key_pos[None, :] <= query_pos[:, None]) & (key_pos[None, :] >= 0)
        wide = allowed[:, None, None, None, :]
        scores = jnp.einsum('tlcqd,kcd->tlcqk', query_block, key_block) * scale
        masked = jnp.where(wide, scores, jnp.float32(-1e+30))
        top = lax.optimization_barrier(jnp.max(masked, axis=-1))
        weights = jnp.where(wide, jnp.exp(masked - top[..., None]), jnp.float32(0.0))
        totals = lax.optimization_barrier(jnp.sum(weights, axis=-1))
        rounded = lax.optimization_barrier(weights.astype(jnp.bfloat16))
        summed = jnp.einsum('tlcqk,kcd->tlcqd', rounded.astype(jnp.float32), val_block)
        result = (summed / totals[..., None]).astype(jnp.bfloat16)
        return result.reshape(TOK_DEV, LAYERS, KV_HEADS * QPER * HD)
    attended = lax.map(one_block, jnp.arange(TOKENS // TOK_DEV, dtype=jnp.int32))
    attended = attended.reshape(TOKENS, LAYERS, KV_HEADS * QPER * HD)
    key_pages = keys.reshape(PAGES, PAGE, KV_HEADS, HD)
    val_pages = values.reshape(PAGES, PAGE, KV_HEADS, HD)
    blocks = jnp.concatenate([key_pages, val_pages], axis=3).transpose(0, 2, 1, 3)
    blocks = blocks.reshape(PAGES * KV_HEADS, PAGE, 2 * HD)
    heads = jnp.arange(KV_HEADS, dtype=jnp.int32)
    target = (page_owner * N_HEAD + heads[None, :] // KV_LOCAL) * SLOTS + page_slot
    cache_pages = jnp.zeros((N_SEQ * N_HEAD * SLOTS, PAGE, 2 * HD), blocks.dtype)
    cache_pages = cache_pages.at[target.reshape(-1).astype(jnp.int32)].set(blocks)
    return (attended, cache_pages)
```

```python
import math

import jax
import jax.numpy as jnp
from jax import lax
from jax.experimental import pallas as pl
from jax.experimental.pallas import tpu as pltpu
from jax.sharding import PartitionSpec as P


QPER = 5
HD = 128
PAGE = 4
CHUNKS = PAGE + 1
NEG = -1e30
F32 = jnp.float32
BF16 = jnp.bfloat16

NT = (((1,), (1,)), ((), ()))
NN = (((1,), (0,)), ((), ()))
TN = (((0,), (0,)), ((), ()))


def dot(a, b, dims=NN):
    return lax.dot_general(a, b, dims, preferred_element_type=F32)


def shifted(x, by):
    count = lax.axis_size("seq")
    pairs = [(i, i + by) for i in range(count - by)]
    return lax.ppermute(x, "seq", pairs)


def block_kernel(keys_ref, vals_ref, out_ref):
    for c in range(2):
        out_ref[c] = keys_ref[:, c * HD : (c + 1) * HD]
        out_ref[2 + c] = vals_ref[:, c * HD : (c + 1) * HD].T


def kv_block(keys, values):
    rows = keys.shape[0]
    return pl.pallas_call(
        block_kernel,
        out_shape=jax.ShapeDtypeStruct((4, HD, rows), BF16),
        name="kv_block",
    )(keys, values)


def pack_kernel(keys_ref, vals_ref, owner_ref, slot_ref, out_ref):
    rows = keys_ref.shape[0]
    pages = rows // PAGE
    per = CHUNKS * 2
    total = out_ref.shape[0]
    page_i = lax.broadcasted_iota(jnp.int32, (pages, rows), 0)
    tok_i = lax.broadcasted_iota(jnp.int32, (pages, rows), 1)
    spread = (tok_i // PAGE == page_i).astype(BF16)
    owner = dot(owner_ref[...].astype(BF16), spread).astype(jnp.int32)
    slot = dot(slot_ref[...].astype(BF16), spread).astype(jnp.int32)
    within = lax.broadcasted_iota(jnp.int32, (1, rows), 1) % PAGE
    keyed, tagged, onehot = [], [], []
    lane_id = lax.broadcasted_iota(jnp.int32, (HD, rows), 0)
    for c in range(2):
        base = owner[c : c + 1] * per
        keyed += [base + within * 2, base + within * 2 + 1]
        tagged.append(jnp.where(within == 0, base + PAGE * 2, -1))
        onehot.append((slot[c : c + 1] == lane_id).astype(BF16))
    parts = []
    for c in range(2):
        parts += [keys_ref[:, c * HD : (c + 1) * HD], vals_ref[:, c * HD : (c + 1) * HD]]
    step = 2 * HD
    for begin in range(0, total, step):
        row = begin + lax.broadcasted_iota(jnp.int32, (step, rows), 0)
        acc = jnp.zeros((step, HD), F32)
        for key, part in zip(keyed, parts):
            acc += dot((row == key).astype(BF16), part)
        for key, hot in zip(tagged, onehot):
            acc += dot((row == key).astype(BF16), hot, NT)
        out_ref[begin : begin + step] = acc.astype(BF16)


def pack_pages(keys, values, owner, slot, seq_count):
    return pl.pallas_call(
        pack_kernel,
        out_shape=jax.ShapeDtypeStruct((seq_count * CHUNKS * 2, HD), BF16),
        name="pack_pages",
    )(keys, values, owner, slot)


def place_kernel(got_ref, out_ref):
    total = got_ref.shape[0]
    per = CHUNKS * 2
    sources = total // per
    slots = out_ref.shape[0] // (PAGE * 2)
    got = got_ref[...]
    src = lax.broadcasted_iota(jnp.int32, (sources, total), 0)
    row = lax.broadcasted_iota(jnp.int32, (sources, total), 1)
    pick = (row == src * per + PAGE * 2).astype(BF16)
    hot = dot(pick, got).astype(BF16)[:, :slots]
    owns = (row // per == src).astype(BF16)
    chosen = dot(hot, owns, TN).astype(BF16)
    dst = lax.broadcasted_iota(jnp.int32, (slots * PAGE * 2, slots), 0)
    slot = lax.broadcasted_iota(jnp.int32, (slots * PAGE * 2, slots), 1)
    wide = dot((dst // (PAGE * 2) == slot).astype(BF16), chosen)
    place = lax.broadcasted_iota(jnp.int32, wide.shape, 0) % (PAGE * 2)
    want = (place % PAGE) * 2 + place // PAGE
    have = lax.broadcasted_iota(jnp.int32, wide.shape, 1) % per
    out_ref[...] = dot(jnp.where(want == have, wide, 0.0).astype(BF16), got).astype(BF16)


def place_pages(got, slots):
    return pl.pallas_call(
        place_kernel,
        out_shape=jax.ShapeDtypeStruct((slots * PAGE * 2, HD), BF16),
        name="place_pages",
    )(got)


def attend_kernel(groups, first, final, *refs):
    refs = list(refs)
    mine_ref, lens_ref, q_ref = refs[:3]
    arrays = 1 + max(g[0] for g in groups)
    kv = refs[3 : 3 + arrays]
    rest = refs[3 + arrays :]
    if not first:
        top_in, tot_in, acc_in = rest[:3]
        rest = rest[3:]
    if final:
        out_ref = rest[0]
        top_ref, tot_ref, acc_ref = rest[1:]
    else:
        top_ref, tot_ref, acc_ref = rest
    rows = q_ref.shape[1]
    head = pl.program_id(0)
    reqs = lens_ref.shape[1]
    base = mine_ref[0] * rows
    lens = jnp.broadcast_to(lens_ref[...], (reqs, reqs)).astype(F32)
    r_i = lax.broadcasted_iota(jnp.int32, (reqs, reqs), 0)
    e_i = lax.broadcasted_iota(jnp.int32, (reqs, reqs), 1)
    starts = jnp.sum(jnp.where(e_i < r_i, lens, 0.0), axis=1, keepdims=True) - base.astype(F32)
    lane = lax.broadcasted_iota(jnp.int32, (1, rows), 1)
    known = jnp.where(starts <= lane.astype(F32), starts, -3e7)
    begin = jnp.max(known, axis=0, keepdims=True).astype(jnp.int32)
    earliest = jnp.min(begin)
    key_i = lax.broadcasted_iota(jnp.int32, (rows, rows), 0)
    qry_i = lax.broadcasted_iota(jnp.int32, (rows, rows), 1)
    factor = math.log2(math.e) / math.sqrt(HD)

    if not first:
        top_ref[...] = top_in[...]
        tot_ref[...] = tot_in[...]
        acc_ref[...] = acc_in[...]

    def block(position, source, index, distance):
        ref = kv[source]
        at = (lambda j: ref[j]) if index is None else (lambda j: ref[index, j])
        k_blk = at(head)
        vt_blk = at(2 + head)
        if distance == 0:
            allowed = (key_i >= begin) & (key_i <= qry_i)
        else:
            allowed = key_i >= begin + distance * rows
        for q in range(QPER):
            queries = q_ref[0, :, q * HD : (q + 1) * HD]
            scores = jnp.where(allowed, dot(k_blk, queries, NT) * factor, NEG)
            best = jnp.max(scores, axis=0, keepdims=True)
            if first and position == 0:
                weights = jnp.exp2(scores - best)
                top_ref[0, 0, q : q + 1] = best
                tot_ref[0, 0, q : q + 1] = jnp.sum(weights, axis=0, keepdims=True)
                acc_ref[0, 0, q] = dot(vt_blk, weights.astype(BF16))
            else:
                old = top_ref[0, 0, q : q + 1]
                fresh = jnp.maximum(old, best)
                shrink = jnp.exp2(old - fresh)
                weights = jnp.exp2(scores - fresh)
                top_ref[0, 0, q : q + 1] = fresh
                tot_ref[0, 0, q : q + 1] = tot_ref[0, 0, q : q + 1] * shrink + jnp.sum(
                    weights, axis=0, keepdims=True
                )
                acc_ref[0, 0, q] = acc_ref[0, 0, q] * shrink + dot(vt_blk, weights.astype(BF16))

    for position, (source, index, distance) in enumerate(groups):
        if distance == 0:
            block(position, source, index, distance)
        else:

            @pl.when(earliest < rows - distance * rows)
            def _(position=position, source=source, index=index, distance=distance):
                block(position, source, index, distance)

    if final:
        for q in range(QPER):
            result = acc_ref[0, 0, q] * (1.0 / tot_ref[0, 0, q : q + 1])
            out_ref[0, :, q * HD : (q + 1) * HD] = result.T.astype(BF16)


def attend(mine, lengths, queries, arrays, groups, state, final):
    layers, rows, width = queries.shape
    heads = width // (QPER * HD)
    first = state is None
    grid = (heads, layers)
    stat = pl.BlockSpec((1, 1, 8, rows), lambda c, l: (c, l, 0, 0))
    accs = pl.BlockSpec((1, 1, QPER, HD, rows), lambda c, l: (c, l, 0, 0, 0))
    q_spec = pl.BlockSpec((1, rows, QPER * HD), lambda c, l: (l, 0, c))
    in_specs = [
        pl.BlockSpec(memory_space=pltpu.SMEM),
        pl.BlockSpec(lengths.shape, lambda c, l: (0, 0)),
        q_spec,
    ]
    for a in arrays:
        in_specs.append(pl.BlockSpec(a.shape, lambda c, l, n=a.ndim: (0,) * n))
    state_shapes = [
        jax.ShapeDtypeStruct((heads, layers, 8, rows), F32),
        jax.ShapeDtypeStruct((heads, layers, 8, rows), F32),
        jax.ShapeDtypeStruct((heads, layers, QPER, HD, rows), F32),
    ]
    operands = [mine, lengths, queries, *arrays]
    if not first:
        in_specs += [stat, stat, accs]
        operands += list(state)
    if final:
        out_shape = jax.ShapeDtypeStruct(queries.shape, BF16)
        out_specs = q_spec
        scratch = [
            pltpu.VMEM((1, 1, 8, rows), F32),
            pltpu.VMEM((1, 1, 8, rows), F32),
            pltpu.VMEM((1, 1, QPER, HD, rows), F32),
        ]
    else:
        out_shape, out_specs, scratch = state_shapes, [stat, stat, accs], []

    def kernel(*refs):
        attend_kernel(groups, first, final, *refs)

    return pl.pallas_call(
        kernel,
        grid=grid,
        in_specs=in_specs,
        out_specs=out_specs,
        out_shape=out_shape,
        scratch_shapes=scratch,
        name="attend_last" if final else "attend_part",
    )(*operands)


def shards(queries, keys, values, lengths, page_owner, page_slot):
    tok_rows = keys.shape[0]
    slots = tok_rows // PAGE * 2
    seq_count = lax.axis_size("seq")
    mine = lax.axis_index("seq").astype(jnp.int32).reshape(1)
    lens = lengths.reshape(1, -1)
    flat_q = queries.transpose(1, 0, 2)

    own = kv_block(keys, values)
    b6 = shifted(own, 6)
    b3 = shifted(own, 3)
    b1 = shifted(own, 1)

    outgoing = pack_pages(keys, values, page_owner.T, page_slot.T, seq_count)
    got = lax.all_to_all(
        outgoing.reshape(seq_count, CHUNKS, 2, HD), "seq", split_axis=0, concat_axis=0, tiled=True
    )

    b247 = shifted(jnp.stack([b1, b3, b6]), 1)
    state = attend(
        mine, lens, flat_q, [own, b1, b3, b6],
        [(0, None, 0), (1, None, 1), (2, None, 3), (3, None, 6)], None, False,
    )
    b58 = shifted(b247[1:], 1)
    state = attend(mine, lens, flat_q, [b247], [(0, 0, 2), (0, 1, 4), (0, 2, 7)], state, False)
    out = attend(mine, lens, flat_q, [b58], [(0, 0, 5), (0, 1, 8)], state, True)
    attended = out.transpose(1, 0, 2)

    placed = place_pages(got.reshape(seq_count * CHUNKS * 2, HD), slots)
    cache_pages = (
        placed.reshape(slots, 2, PAGE, HD).transpose(0, 2, 1, 3).reshape(slots, PAGE, 2 * HD)
    )
    return (attended, cache_pages)


def solution(mesh):
    placed = (
        P(("group", "seq"), None, "head"),
        P(("group", "seq"), "head"),
        P(("group", "seq"), "head"),
        P("group"),
        P(("group", "seq"), "head"),
        P(("group", "seq"), "head"),
    )
    return jax.shard_map(
        shards,
        mesh=mesh,
        in_specs=placed,
        out_specs=(P(("group", "seq"), None, "head"), P(("group", "seq", "head"), None, None)),
        check_vma=False,
    )
```

```python
import math

import jax
import jax.numpy as jnp
from jax import lax
from jax.experimental import pallas as pl
from jax.experimental.pallas import tpu as pltpu
from jax.sharding import PartitionSpec as P


QPER = 5
HD = 128
PAGE = 4
CHUNKS = PAGE + 1
NEG = -1e30
WIDE = 5
F32 = jnp.float32
BF16 = jnp.bfloat16

NT = (((1,), (1,)), ((), ()))
NN = (((1,), (0,)), ((), ()))
TN = (((0,), (0,)), ((), ()))


def dot(a, b, dims=NN):
    return lax.dot_general(a, b, dims, preferred_element_type=F32)


def shifted(x, by):
    count = lax.axis_size("seq")
    pairs = [(i, i + by) for i in range(count - by)]
    return lax.ppermute(x, "seq", pairs)


def near_core(x):
    return pltpu.with_memory_space_constraint(x, pltpu.VMEM)


def pack_kernel(keys_ref, vals_ref, owner_ref, slot_ref, own_ref, out_ref):
    for c in range(2):
        own_ref[c] = keys_ref[:, c * HD : (c + 1) * HD]
        own_ref[2 + c] = vals_ref[:, c * HD : (c + 1) * HD].T
    rows = keys_ref.shape[0]
    pages = rows // PAGE
    per = CHUNKS * 2
    total = out_ref.shape[0]
    page_i = lax.broadcasted_iota(jnp.int32, (pages, rows), 0)
    tok_i = lax.broadcasted_iota(jnp.int32, (pages, rows), 1)
    spread = (tok_i // PAGE == page_i).astype(BF16)
    owner = dot(owner_ref[...].astype(BF16), spread).astype(jnp.int32)
    slot = dot(slot_ref[...].astype(BF16), spread).astype(jnp.int32)
    within = lax.broadcasted_iota(jnp.int32, (1, rows), 1) % PAGE
    keyed, tagged, onehot = [], [], []
    lane_id = lax.broadcasted_iota(jnp.int32, (HD, rows), 0)
    for c in range(2):
        base = owner[c : c + 1] * per
        keyed += [base + within * 2, base + within * 2 + 1]
        tagged.append(jnp.where(within == 0, base + PAGE * 2, -1))
        onehot.append((slot[c : c + 1] == lane_id).astype(BF16))
    parts = []
    for c in range(2):
        parts += [keys_ref[:, c * HD : (c + 1) * HD], vals_ref[:, c * HD : (c + 1) * HD]]
    step = 2 * HD
    for begin in range(0, total, step):
        row = begin + lax.broadcasted_iota(jnp.int32, (step, rows), 0)
        acc = jnp.zeros((step, HD), F32)
        for key, part in zip(keyed, parts):
            acc += dot((row == key).astype(BF16), part)
        for key, hot in zip(tagged, onehot):
            acc += dot((row == key).astype(BF16), hot, NT)
        out_ref[begin : begin + step] = acc.astype(BF16)


def pack_pages(keys, values, owner, slot, seq_count):
    return pl.pallas_call(
        pack_kernel,
        out_shape=(
            pltpu.VMEM((4, HD, keys.shape[0]), BF16),
            pltpu.VMEM((seq_count * CHUNKS * 2, HD), BF16),
        ),
        name="pack_pages",
    )(keys, values, owner, slot)


def place_kernel(got_ref, out_ref):
    total = got_ref.shape[0]
    per = CHUNKS * 2
    sources = total // per
    pages = PAGE * 2
    slots = out_ref.shape[0] // pages
    got = got_ref[...]
    row = lax.broadcasted_iota(jnp.int32, (1, total), 1)
    source, inside = row // per, row % per
    src = lax.broadcasted_iota(jnp.int32, (sources, 1), 0)
    hot = dot((row == src * per + pages).astype(BF16), got).astype(BF16)[:, :slots]
    chosen = dot(hot, (source == src).astype(BF16), TN).astype(BF16)
    dst = lax.broadcasted_iota(jnp.int32, (slots * pages, 1), 0)
    slot = lax.broadcasted_iota(jnp.int32, (1, slots), 1)
    wide = dot((dst // pages == slot).astype(BF16), chosen).astype(BF16)
    want = (dst % PAGE) * 2 + dst % pages // PAGE
    step = 2 * HD
    for begin in range(0, slots * pages, step):
        here = slice(begin, begin + step)
        placed = jnp.where(want[here] == inside, wide[here], jnp.zeros((), BF16))
        out_ref[here] = dot(placed, got).astype(BF16)


def place_pages(got, slots):
    return pl.pallas_call(
        place_kernel,
        out_shape=jax.ShapeDtypeStruct((slots * PAGE * 2, HD), BF16),
        name="place_pages",
    )(near_core(got))


def attend_kernel(groups, first, final, *refs):
    refs = list(refs)
    mine_ref, lens_ref, q_ref = refs[:3]
    arrays = 1 + max(g[0] for g in groups)
    kv = refs[3 : 3 + arrays]
    rest = refs[3 + arrays :]
    if not first:
        top_in, tot_in, acc_in = rest[:3]
        rest = rest[3:]
    if final:
        (out_ref,) = rest
    else:
        top_ref, tot_ref, acc_ref = rest
    rows = q_ref.shape[1]
    head = pl.program_id(0)
    reqs = lens_ref.shape[1]
    base = mine_ref[0] * rows
    lens = jnp.broadcast_to(lens_ref[...], (reqs, reqs)).astype(F32)
    r_i = lax.broadcasted_iota(jnp.int32, (reqs, reqs), 0)
    e_i = lax.broadcasted_iota(jnp.int32, (reqs, reqs), 1)
    starts = jnp.sum(jnp.where(e_i < r_i, lens, 0.0), axis=1, keepdims=True) - base.astype(F32)
    lane = lax.broadcasted_iota(jnp.int32, (1, rows), 1)
    known = jnp.where(starts <= lane.astype(F32), starts, -3e7)
    begin = jnp.max(known, axis=0, keepdims=True).astype(jnp.int32)
    earliest = jnp.min(begin)
    factor = math.log2(math.e) / math.sqrt(HD)

    key_i = lax.broadcasted_iota(jnp.int32, (rows, rows), 0)
    qry_i = lax.broadcasted_iota(jnp.int32, (rows, rows), 1)

    def take(some):
        keys, vals, masks = [], [], []
        for source, index, distance in some:
            ref = kv[source]
            keys.append(ref[head] if index is None else ref[index, head])
            vals.append(ref[2 + head] if index is None else ref[index, 2 + head])
            inside = key_i >= begin + distance * rows
            masks.append(inside & (key_i <= qry_i) if distance == 0 else inside)
        k_all = jnp.concatenate(keys, axis=0)
        v_all = jnp.concatenate(vals, axis=1)
        allowed = jnp.concatenate(masks, axis=0)
        for begin_q in range(0, QPER, WIDE):
            heads = range(begin_q, min(begin_q + WIDE, QPER))
            lanes = slice(heads[0] * rows, (heads[-1] + 1) * rows)
            queries = jnp.concatenate([q_ref[0, :, q * HD : (q + 1) * HD] for q in heads], axis=0)
            scores = dot(k_all, queries, NT) * factor
            scores = jnp.where(jnp.concatenate([allowed] * len(heads), axis=1), scores, NEG)
            top = jnp.max(scores, axis=0, keepdims=True)
            if first:
                weights = jnp.exp2(scores - top)
                total = jnp.sum(weights, axis=0, keepdims=True)
                acc = dot(v_all, weights.astype(BF16))
            else:
                old = top_in[0, 0, 0:1, lanes]
                top = jnp.maximum(old, top)
                shrink = jnp.exp2(old - top)
                weights = jnp.exp2(scores - top)
                total = tot_in[0, 0, 0:1, lanes] * shrink + jnp.sum(weights, axis=0, keepdims=True)
                acc = acc_in[0, 0, :, lanes] * shrink + dot(v_all, weights.astype(BF16))
            if final:
                result = acc * (1.0 / total)
                for i, q in enumerate(heads):
                    piece = result[:, i * rows : (i + 1) * rows]
                    out_ref[0, :, q * HD : (q + 1) * HD] = piece.T.astype(BF16)
            else:
                top_ref[0, 0, 0:1, lanes] = top
                tot_ref[0, 0, 0:1, lanes] = total
                acc_ref[0, 0, :, lanes] = acc

    def skip():
        for q in range(QPER):
            lanes = slice(q * rows, (q + 1) * rows)
            if final:
                result = acc_in[0, 0, :, lanes] * (1.0 / tot_in[0, 0, 0:1, lanes])
                out_ref[0, :, q * HD : (q + 1) * HD] = result.T.astype(BF16)
            else:
                top_ref[0, 0, 0:1, lanes] = top_in[0, 0, 0:1, lanes]
                tot_ref[0, 0, 0:1, lanes] = tot_in[0, 0, 0:1, lanes]
                acc_ref[0, 0, :, lanes] = acc_in[0, 0, :, lanes]

    for used in range(1 if first else 0, len(groups) + 1):
        some = groups[:used]
        needed = used < 1 or earliest < rows - some[-1][2] * rows
        further = used < len(groups) and earliest < rows - groups[used][2] * rows
        case = True
        if used and some[-1][2]:
            case = needed
        if used < len(groups):
            case = jnp.logical_and(case, jnp.logical_not(further))
        pl.when(case)(lambda some=some: take(some) if some else skip())


def attend(mine, lengths, queries, arrays, groups, state, final):
    layers, rows, width = queries.shape
    heads = width // (QPER * HD)
    first = state is None
    grid = (heads, layers)
    stat = pl.BlockSpec((1, 1, 8, QPER * rows), lambda c, l: (c, l, 0, 0))
    accs = pl.BlockSpec((1, 1, HD, QPER * rows), lambda c, l: (c, l, 0, 0))
    q_spec = pl.BlockSpec((1, rows, QPER * HD), lambda c, l: (l, 0, c))
    in_specs = [
        pl.BlockSpec(memory_space=pltpu.SMEM),
        pl.BlockSpec(lengths.shape, lambda c, l: (0, 0)),
        q_spec,
    ]
    in_specs += [pl.BlockSpec(memory_space=pltpu.VMEM) for _ in arrays]
    state_shapes = [
        jax.ShapeDtypeStruct((heads, layers, 8, QPER * rows), F32),
        jax.ShapeDtypeStruct((heads, layers, 8, QPER * rows), F32),
        jax.ShapeDtypeStruct((heads, layers, HD, QPER * rows), F32),
    ]
    operands = [mine, lengths, queries, *map(near_core, arrays)]
    if not first:
        in_specs += [stat, stat, accs]
        operands += list(state)
    if final:
        out_shape = jax.ShapeDtypeStruct(queries.shape, BF16)
        out_specs = q_spec
    else:
        out_shape, out_specs = state_shapes, [stat, stat, accs]

    def kernel(*refs):
        attend_kernel(groups, first, final, *refs)

    return pl.pallas_call(
        kernel,
        grid=grid,
        in_specs=in_specs,
        out_specs=out_specs,
        out_shape=out_shape,
        name="attend_last" if final else "attend_part",
    )(*operands)


def shards(queries, keys, values, lengths, page_owner, page_slot):
    tok_rows = keys.shape[0]
    slots = tok_rows // PAGE * 2
    seq_count = lax.axis_size("seq")
    mine = lax.axis_index("seq").astype(jnp.int32).reshape(1)
    lens = lengths.reshape(1, -1)
    flat_q = queries.transpose(1, 0, 2)

    own, outgoing = pack_pages(keys, values, page_owner.T, page_slot.T, seq_count)
    b6 = shifted(own, 6)
    b3 = shifted(own, 3)
    b1 = shifted(own, 1)

    got = lax.all_to_all(
        outgoing.reshape(seq_count, CHUNKS, 2, HD), "seq", split_axis=0, concat_axis=0, tiled=True
    )

    b47 = shifted(jnp.stack([b3, b6]), 1)
    b2 = shifted(b1, 1)
    groups = [(0, None, 0), (1, None, 1), (2, None, 3), (3, None, 6)]
    state = attend(mine, lens, flat_q, [own, b1, b3, b6], groups, None, False)
    b58 = shifted(b47, 1)
    groups = [(0, None, 2), (1, 0, 4), (1, 1, 7)]
    state = attend(mine, lens, flat_q, [b2, b47], groups, state, False)
    out = attend(mine, lens, flat_q, [b58], [(0, 0, 5), (0, 1, 8)], state, True)
    attended = out.transpose(1, 0, 2)

    placed = place_pages(got.reshape(seq_count * CHUNKS * 2, HD), slots)
    cache_pages = (
        placed.reshape(slots, 2, PAGE, HD).transpose(0, 2, 1, 3).reshape(slots, PAGE, 2 * HD)
    )
    return (attended, cache_pages)


def solution(mesh):
    placed = (
        P(("group", "seq"), None, "head"),
        P(("group", "seq"), "head"),
        P(("group", "seq"), "head"),
        P("group"),
        P(("group", "seq"), "head"),
        P(("group", "seq"), "head"),
    )
    return jax.shard_map(
        shards,
        mesh=mesh,
        in_specs=placed,
        out_specs=(P(("group", "seq"), None, "head"), P(("group", "seq", "head"), None, None)),
        check_vma=False,
    )
```

```python
import math

import jax
import jax.numpy as jnp
from jax import lax
from jax.experimental import pallas as pl
from jax.experimental.pallas import tpu as pltpu
from jax.sharding import PartitionSpec as P


QPER = 5
HD = 128
PAGE = 4
CHUNKS = PAGE + 1
NEG = -1e30
PAIR = 2
F32 = jnp.float32
BF16 = jnp.bfloat16

NT = (((1,), (1,)), ((), ()))
NN = (((1,), (0,)), ((), ()))
TN = (((0,), (0,)), ((), ()))


def dot(a, b, dims=NN):
    return lax.dot_general(a, b, dims, preferred_element_type=F32)


def shifted(x, by):
    count = lax.axis_size("seq")
    pairs = [(i, i + by) for i in range(count - by)]
    return lax.ppermute(x, "seq", pairs)


def near_core(x):
    return pltpu.with_memory_space_constraint(x, pltpu.VMEM)


def pack_kernel(keys_ref, vals_ref, owner_ref, slot_ref, own_ref, out_ref):
    for c in range(2):
        own_ref[c * HD : (c + 1) * HD] = keys_ref[:, c * HD : (c + 1) * HD]
        own_ref[(2 + c) * HD : (3 + c) * HD] = vals_ref[:, c * HD : (c + 1) * HD].T
    rows = keys_ref.shape[0]
    pages = rows // PAGE
    per = CHUNKS * 2
    total = out_ref.shape[0]
    page_i = lax.broadcasted_iota(jnp.int32, (pages, rows), 0)
    tok_i = lax.broadcasted_iota(jnp.int32, (pages, rows), 1)
    spread = (tok_i // PAGE == page_i).astype(BF16)
    owner = dot(owner_ref[...].astype(BF16), spread).astype(jnp.int32)
    slot = dot(slot_ref[...].astype(BF16), spread).astype(jnp.int32)
    within = lax.broadcasted_iota(jnp.int32, (1, rows), 1) % PAGE
    keyed, tagged, onehot = [], [], []
    lane_id = lax.broadcasted_iota(jnp.int32, (HD, rows), 0)
    for c in range(2):
        base = owner[c : c + 1] * per
        keyed += [base + within * 2, base + within * 2 + 1]
        tagged.append(jnp.where(within == 0, base + PAGE * 2, -1))
        onehot.append((slot[c : c + 1] == lane_id).astype(BF16))
    parts = []
    for c in range(2):
        parts += [keys_ref[:, c * HD : (c + 1) * HD], vals_ref[:, c * HD : (c + 1) * HD]]
    step = 2 * HD
    for begin in range(0, total, step):
        row = begin + lax.broadcasted_iota(jnp.int32, (step, rows), 0)
        acc = jnp.zeros((step, HD), F32)
        for key, part in zip(keyed, parts):
            acc += dot((row == key).astype(BF16), part)
        for key, hot in zip(tagged, onehot):
            acc += dot((row == key).astype(BF16), hot, NT)
        out_ref[begin : begin + step] = acc.astype(BF16)


def pack_pages(keys, values, owner, slot, seq_count):
    return pl.pallas_call(
        pack_kernel,
        out_shape=(
            pltpu.VMEM((4 * HD, keys.shape[0]), BF16),
            pltpu.VMEM((seq_count * CHUNKS * 2, HD), BF16),
        ),
        name="pack_pages",
    )(keys, values, owner, slot)


def place_kernel(got_ref, out_ref):
    total = got_ref.shape[0]
    per = CHUNKS * 2
    sources = total // per
    pages = PAGE * 2
    slots = out_ref.shape[0] // pages
    got = got_ref[...]
    row = lax.broadcasted_iota(jnp.int32, (1, total), 1)
    source, inside = row // per, row % per
    src = lax.broadcasted_iota(jnp.int32, (sources, 1), 0)
    hot = dot((row == src * per + pages).astype(BF16), got).astype(BF16)[:, :slots]
    chosen = dot(hot, (source == src).astype(BF16), TN).astype(BF16)
    dst = lax.broadcasted_iota(jnp.int32, (slots * pages, 1), 0)
    slot = lax.broadcasted_iota(jnp.int32, (1, slots), 1)
    wide = dot((dst // pages == slot).astype(BF16), chosen).astype(BF16)
    want = (dst % PAGE) * 2 + dst % pages // PAGE
    step = 2 * HD
    for begin in range(0, slots * pages, step):
        here = slice(begin, begin + step)
        placed = jnp.where(want[here] == inside, wide[here], jnp.zeros((), BF16))
        out_ref[here] = dot(placed, got).astype(BF16)


def place_pages(got, slots):
    return pl.pallas_call(
        place_kernel,
        out_shape=jax.ShapeDtypeStruct((slots * PAGE * 2, HD), BF16),
        name="place_pages",
    )(near_core(got))


def attend_kernel(groups, first, final, *refs):
    refs = list(refs)
    mine_ref, lens_ref, q_ref = refs[:3]
    arrays = 1 + max(g[0] for g in groups)
    kv = refs[3 : 3 + arrays]
    rest = refs[3 + arrays :]
    state_in = None if first else rest.pop(0)
    result_ref = rest.pop(0)
    work, sems = rest[:2]
    staged = rest[2] if final else None
    layers, rows, width = q_ref.shape
    wide = QPER * HD
    units = layers * width // wide
    reqs = lens_ref.shape[1]

    def fetch(i):
        return pltpu.make_async_copy(state_in.at[i], work.at[i], sems.at[0, i])

    def send(i):
        if not final:
            return pltpu.make_async_copy(work.at[i], result_ref.at[i], sems.at[1, i])
        lanes = pl.ds(pl.multiple_of(i % (width // wide) * wide, HD), wide)
        return pltpu.make_async_copy(
            staged.at[i], result_ref.at[i // (width // wide), :, lanes], sems.at[1, i]
        )

    if not first:
        for i in range(units):
            fetch(i).start()

    base = mine_ref[0] * rows
    lens = jnp.broadcast_to(lens_ref[...], (reqs, reqs)).astype(F32)
    r_i = lax.broadcasted_iota(jnp.int32, (reqs, reqs), 0)
    e_i = lax.broadcasted_iota(jnp.int32, (reqs, reqs), 1)
    starts = jnp.sum(jnp.where(e_i < r_i, lens, 0.0), axis=1, keepdims=True) - base.astype(F32)
    lane = lax.broadcasted_iota(jnp.int32, (1, rows), 1)
    known = jnp.where(starts <= lane.astype(F32), starts, -3e7)
    begin = jnp.max(known, axis=0, keepdims=True).astype(jnp.int32)
    earliest = jnp.min(begin)
    factor = math.log2(math.e) / math.sqrt(HD)

    def take(some, i):
        head = i % (width // wide)
        layer = i // (width // wide)
        if not first:
            old = work[i, HD : HD + 1]
            old_total = work[i, HD + 8 : HD + 9]
        if some:
            key_i = lax.broadcasted_iota(jnp.int32, (rows, rows), 0)
            qry_i = lax.broadcasted_iota(jnp.int32, (rows, rows), 1)
            keys, vals, masks = [], [], []
            for source, index, distance in some:
                at = pl.multiple_of((4 * index + head) * HD, HD)
                keys.append(kv[source][pl.ds(at, HD)])
                vals.append(kv[source][pl.ds(at + 2 * HD, HD)])
                inside = key_i >= begin + distance * rows
                masks.append(inside & (key_i <= qry_i) if distance == 0 else inside)
            v_all = jnp.concatenate(vals, axis=1)
            lanes = [pl.ds(pl.multiple_of((head * QPER + q) * HD, HD), HD) for q in range(QPER)]
            queries = jnp.concatenate([q_ref[layer, :, at] for at in lanes], axis=0)
            scores = dot(jnp.concatenate(keys, axis=0), queries, NT) * factor
            allowed = jnp.concatenate([jnp.concatenate(masks, axis=0)] * QPER, axis=1)
            scores = jnp.where(allowed, scores, NEG)
            top = jnp.max(scores, axis=0, keepdims=True)
            if not first:
                top = jnp.maximum(old, top)
            weights = jnp.exp2(scores - top)
            total = jnp.sum(weights, axis=0, keepdims=True)
            acc = dot(v_all, weights.astype(BF16))
            if not first:
                shrink = jnp.exp2(old - top)
                total += old_total * shrink
                acc += work[i, :HD] * shrink
        if final:
            if not some:
                total, acc = old_total, work[i, :HD]
            normed = (acc * (1.0 / total)).astype(BF16)
            for q in range(QPER):
                staged[i, :, q * HD : (q + 1) * HD] = normed[:, q * rows : (q + 1) * rows].T
        elif some:
            work[i, :HD] = acc
            work[i, HD : HD + 8] = jnp.broadcast_to(top, (8, wide))
            work[i, HD + 8 :] = jnp.broadcast_to(total, (8, wide))

    for used in range(1 if first else 0, len(groups) + 1):
        some = groups[:used]
        case = True
        if used and some[-1][2]:
            case = earliest < rows - some[-1][2] * rows
        if used < len(groups):
            case = jnp.logical_and(case, earliest >= rows - groups[used][2] * rows)

        @pl.when(case)
        def _(some=some):
            @pl.loop(0, units, step=PAIR)
            def _(i):
                for j in range(PAIR):
                    if not first:
                        fetch(i + j).wait()
                for j in range(PAIR):
                    take(some, i + j)
                for j in range(PAIR):
                    send(i + j).start()

    for i in range(units):
        send(i).wait()


def attend(mine, lengths, queries, arrays, groups, state, final):
    layers, rows, width = queries.shape
    units = layers * width // (QPER * HD)
    first = state is None
    in_specs = [
        pl.BlockSpec(memory_space=pltpu.SMEM),
        pl.BlockSpec(memory_space=pltpu.VMEM),
        pl.BlockSpec(memory_space=pltpu.VMEM),
    ]
    in_specs += [pl.BlockSpec(memory_space=pltpu.VMEM) for _ in arrays]
    kept = (units, HD + 16, QPER * rows)
    operands = [mine, lengths, near_core(queries), *map(near_core, arrays)]
    if not first:
        in_specs.append(pl.BlockSpec(memory_space=pl.ANY))
        operands.append(state)
    scratch = [pltpu.VMEM(kept, F32), pltpu.SemaphoreType.DMA((2, units))]
    if final:
        scratch.append(pltpu.VMEM((units, rows, QPER * HD), BF16))
        out_shape = jax.ShapeDtypeStruct(queries.shape, BF16)
    else:
        out_shape = jax.ShapeDtypeStruct(kept, F32)

    def kernel(*refs):
        attend_kernel(groups, first, final, *refs)

    return pl.pallas_call(
        kernel,
        in_specs=in_specs,
        out_specs=pl.BlockSpec(memory_space=pl.ANY),
        out_shape=out_shape,
        scratch_shapes=scratch,
        name="attend_last" if final else "attend_part",
    )(*operands)


def shards(queries, keys, values, lengths, page_owner, page_slot):
    tok_rows = keys.shape[0]
    slots = tok_rows // PAGE * 2
    seq_count = lax.axis_size("seq")
    mine = lax.axis_index("seq").astype(jnp.int32).reshape(1)
    lens = lengths.reshape(1, -1)
    flat_q = queries.transpose(1, 0, 2)

    own, outgoing = pack_pages(keys, values, page_owner.T, page_slot.T, seq_count)
    b6 = shifted(own, 6)
    b3 = shifted(own, 3)
    b1 = shifted(own, 1)

    got = lax.all_to_all(
        outgoing.reshape(seq_count, CHUNKS, 2, HD), "seq", split_axis=0, concat_axis=0, tiled=True
    )

    b47 = shifted(jnp.concatenate([b3, b6]), 1)
    b2 = shifted(b1, 1)
    groups = [(0, 0, 0), (1, 0, 1), (2, 0, 3), (3, 0, 6)]
    state = attend(mine, lens, flat_q, [own, b1, b3, b6], groups, None, False)
    b58 = shifted(b47, 1)
    groups = [(0, 0, 2), (1, 0, 4), (1, 1, 7)]
    state = attend(mine, lens, flat_q, [b2, b47], groups, state, False)
    out = attend(mine, lens, flat_q, [b58], [(0, 0, 5), (0, 1, 8)], state, True)
    attended = out.transpose(1, 0, 2)

    placed = place_pages(got.reshape(seq_count * CHUNKS * 2, HD), slots)
    cache_pages = (
        placed.reshape(slots, 2, PAGE, HD).transpose(0, 2, 1, 3).reshape(slots, PAGE, 2 * HD)
    )
    return (attended, cache_pages)


def solution(mesh):
    placed = (
        P(("group", "seq"), None, "head"),
        P(("group", "seq"), "head"),
        P(("group", "seq"), "head"),
        P("group"),
        P(("group", "seq"), "head"),
        P(("group", "seq"), "head"),
    )
    return jax.shard_map(
        shards,
        mesh=mesh,
        in_specs=placed,
        out_specs=(P(("group", "seq"), None, "head"), P(("group", "seq", "head"), None, None)),
        check_vma=False,
    )
```

```python
import math

import jax
import jax.numpy as jnp
from jax import lax
from jax.experimental import pallas as pl
from jax.experimental.pallas import tpu as pltpu
from jax.sharding import PartitionSpec as P


QPER = 5
HD = 128
PAGE = 4
CHUNKS = PAGE + 1
NEG = -1e30
PAIR = 2
F32 = jnp.float32
BF16 = jnp.bfloat16

NT = (((1,), (1,)), ((), ()))
NN = (((1,), (0,)), ((), ()))
TN = (((0,), (0,)), ((), ()))


def dot(a, b, dims=NN):
    return lax.dot_general(a, b, dims, preferred_element_type=F32)


def shifted(x, by):
    count = lax.axis_size("seq")
    pairs = [(i, i + by) for i in range(count - by)]
    return lax.ppermute(x, "seq", pairs)


def near_core(x):
    return pltpu.with_memory_space_constraint(x, pltpu.VMEM)


def pack_kernel(keys_ref, vals_ref, owner_ref, slot_ref, own_ref, out_ref):
    for c in range(2):
        own_ref[c * HD : (c + 1) * HD] = keys_ref[:, c * HD : (c + 1) * HD]
        own_ref[(2 + c) * HD : (3 + c) * HD] = vals_ref[:, c * HD : (c + 1) * HD].T
    rows = keys_ref.shape[0]
    pages = rows // PAGE
    per = CHUNKS * 2
    total = out_ref.shape[0]
    page_i = lax.broadcasted_iota(jnp.int32, (pages, rows), 0)
    tok_i = lax.broadcasted_iota(jnp.int32, (pages, rows), 1)
    spread = (tok_i // PAGE == page_i).astype(BF16)
    owner = dot(owner_ref[...].astype(BF16), spread).astype(jnp.int32)
    slot = dot(slot_ref[...].astype(BF16), spread).astype(jnp.int32)
    within = lax.broadcasted_iota(jnp.int32, (1, rows), 1) % PAGE
    keyed, tagged, onehot = [], [], []
    lane_id = lax.broadcasted_iota(jnp.int32, (HD, rows), 0)
    for c in range(2):
        base = owner[c : c + 1] * per
        keyed += [base + within * 2, base + within * 2 + 1]
        tagged.append(jnp.where(within == 0, base + PAGE * 2, -1))
        onehot.append((slot[c : c + 1] == lane_id).astype(BF16))
    parts = []
    for c in range(2):
        parts += [keys_ref[:, c * HD : (c + 1) * HD], vals_ref[:, c * HD : (c + 1) * HD]]
    step = 2 * HD
    for begin in range(0, total, step):
        row = begin + lax.broadcasted_iota(jnp.int32, (step, rows), 0)
        acc = jnp.zeros((step, HD), F32)
        for key, part in zip(keyed, parts):
            acc += dot((row == key).astype(BF16), part)
        for key, hot in zip(tagged, onehot):
            acc += dot((row == key).astype(BF16), hot, NT)
        out_ref[begin : begin + step] = acc.astype(BF16)


def pack_pages(keys, values, owner, slot, seq_count):
    return pl.pallas_call(
        pack_kernel,
        out_shape=(
            pltpu.VMEM((4 * HD, keys.shape[0]), BF16),
            pltpu.VMEM((seq_count * CHUNKS * 2, HD), BF16),
        ),
        name="pack_pages",
    )(keys, values, owner, slot)


def place_pages(got_ref, out_ref):
    total = got_ref.shape[0]
    per = CHUNKS * 2
    sources = total // per
    pages = PAGE * 2
    slots = out_ref.shape[0] // pages
    got = got_ref[...]
    row = lax.broadcasted_iota(jnp.int32, (1, total), 1)
    source, inside = row // per, row % per
    src = lax.broadcasted_iota(jnp.int32, (sources, 1), 0)
    hot = dot((row == src * per + pages).astype(BF16), got).astype(BF16)[:, :slots]
    chosen = dot(hot, (source == src).astype(BF16), TN).astype(BF16)
    dst = lax.broadcasted_iota(jnp.int32, (slots * pages, 1), 0)
    slot = lax.broadcasted_iota(jnp.int32, (1, slots), 1)
    wide = dot((dst // pages == slot).astype(BF16), chosen).astype(BF16)
    want = (dst % PAGE) * 2 + dst % pages // PAGE
    step = 2 * HD
    for begin in range(0, slots * pages, step):
        here = slice(begin, begin + step)
        placed = jnp.where(want[here] == inside, wide[here], jnp.zeros((), BF16))
        out_ref[here] = dot(placed, got).astype(BF16)


def attend_kernel(groups, first, final, *refs):
    refs = list(refs)
    mine_ref, lens_ref, q_ref = refs[:3]
    arrays = 1 + max(g[0] for g in groups)
    kv = refs[3 : 3 + arrays]
    rest = refs[3 + arrays :]
    state_in = None if first else rest.pop(0)
    if final:
        got_ref, result_ref, pages_ref, work, sems, staged, placed, page_sem = rest
    else:
        result_ref, work, sems = rest
    layers, rows, width = q_ref.shape
    wide = QPER * HD
    units = layers * width // wide
    reqs = lens_ref.shape[1]

    def fetch(i):
        return pltpu.make_async_copy(state_in.at[i], work.at[i], sems.at[0, i])

    def send(i):
        if not final:
            return pltpu.make_async_copy(work.at[i], result_ref.at[i], sems.at[1, i])
        lanes = pl.ds(pl.multiple_of(i % (width // wide) * wide, HD), wide)
        return pltpu.make_async_copy(
            staged.at[i], result_ref.at[i // (width // wide), :, lanes], sems.at[1, i]
        )

    if not first:
        for i in range(units):
            fetch(i).start()
    if final:
        place_pages(got_ref, placed)
        pages_out = pltpu.make_async_copy(placed, pages_ref, page_sem)
        pages_out.start()

    base = mine_ref[0] * rows
    lens = jnp.broadcast_to(lens_ref[...], (reqs, reqs)).astype(F32)
    r_i = lax.broadcasted_iota(jnp.int32, (reqs, reqs), 0)
    e_i = lax.broadcasted_iota(jnp.int32, (reqs, reqs), 1)
    starts = jnp.sum(jnp.where(e_i < r_i, lens, 0.0), axis=1, keepdims=True) - base.astype(F32)
    lane = lax.broadcasted_iota(jnp.int32, (1, rows), 1)
    known = jnp.where(starts <= lane.astype(F32), starts, -3e7)
    begin = jnp.max(known, axis=0, keepdims=True).astype(jnp.int32)
    earliest = jnp.min(begin)
    factor = math.log2(math.e) / math.sqrt(HD)

    def take(some, i):
        head = i % (width // wide)
        layer = i // (width // wide)
        if not first:
            old = work[i, HD : HD + 1]
            old_total = work[i, HD + 8 : HD + 9]
        if some:
            key_i = lax.broadcasted_iota(jnp.int32, (rows, rows), 0)
            qry_i = lax.broadcasted_iota(jnp.int32, (rows, rows), 1)
            keys, vals, masks = [], [], []
            for source, index, distance in some:
                at = pl.multiple_of((4 * index + head) * HD, HD)
                keys.append(kv[source][pl.ds(at, HD)])
                vals.append(kv[source][pl.ds(at + 2 * HD, HD)])
                inside = key_i >= begin + distance * rows
                masks.append(inside & (key_i <= qry_i) if distance == 0 else inside)
            v_all = jnp.concatenate(vals, axis=1)
            lanes = [pl.ds(pl.multiple_of((head * QPER + q) * HD, HD), HD) for q in range(QPER)]
            queries = jnp.concatenate([q_ref[layer, :, at] for at in lanes], axis=0)
            scores = dot(jnp.concatenate(keys, axis=0), queries, NT) * factor
            allowed = jnp.concatenate([jnp.concatenate(masks, axis=0)] * QPER, axis=1)
            scores = jnp.where(allowed, scores, NEG)
            top = jnp.max(scores, axis=0, keepdims=True)
            if not first:
                top = jnp.maximum(old, top)
            weights = jnp.exp2(scores - top)
            total = jnp.sum(weights, axis=0, keepdims=True)
            acc = dot(v_all, weights.astype(BF16))
            if not first:
                shrink = jnp.exp2(old - top)
                total += old_total * shrink
                acc += work[i, :HD] * shrink
        if final:
            if not some:
                total, acc = old_total, work[i, :HD]
            normed = (acc * (1.0 / total)).astype(BF16)
            for q in range(QPER):
                staged[i, :, q * HD : (q + 1) * HD] = normed[:, q * rows : (q + 1) * rows].T
        elif some:
            work[i, :HD] = acc
            work[i, HD : HD + 8] = jnp.broadcast_to(top, (8, wide))
            work[i, HD + 8 :] = jnp.broadcast_to(total, (8, wide))

    for used in range(1 if first else 0, len(groups) + 1):
        some = groups[:used]
        case = True
        if used and some[-1][2]:
            case = earliest < rows - some[-1][2] * rows
        if used < len(groups):
            case = jnp.logical_and(case, earliest >= rows - groups[used][2] * rows)

        @pl.when(case)
        def _(some=some):
            @pl.loop(0, units, step=PAIR)
            def _(i):
                for j in range(PAIR):
                    if not first:
                        fetch(i + j).wait()
                for j in range(PAIR):
                    take(some, i + j)
                for j in range(PAIR):
                    send(i + j).start()

    for i in range(units):
        send(i).wait()
    if final:
        pages_out.wait()


def attend(mine, lengths, queries, arrays, groups, state, got=None):
    layers, rows, width = queries.shape
    units = layers * width // (QPER * HD)
    first, final = state is None, got is not None
    in_specs = [
        pl.BlockSpec(memory_space=pltpu.SMEM),
        pl.BlockSpec(memory_space=pltpu.VMEM),
        pl.BlockSpec(memory_space=pltpu.VMEM),
    ]
    in_specs += [pl.BlockSpec(memory_space=pltpu.VMEM) for _ in arrays]
    kept = (units, HD + 16, QPER * rows)
    operands = [mine, lengths, near_core(queries), *map(near_core, arrays)]
    if not first:
        in_specs.append(pl.BlockSpec(memory_space=pl.ANY))
        operands.append(state)
    scratch = [pltpu.VMEM(kept, F32), pltpu.SemaphoreType.DMA((2, units))]
    hbm = pl.BlockSpec(memory_space=pl.ANY)
    if final:
        in_specs.append(pl.BlockSpec(memory_space=pltpu.VMEM))
        operands.append(near_core(got))
        pages = (rows // PAGE * 2 * PAGE * 2, HD)
        scratch += [
            pltpu.VMEM((units, rows, QPER * HD), BF16),
            pltpu.VMEM(pages, BF16),
            pltpu.SemaphoreType.DMA,
        ]
        out_shape = (jax.ShapeDtypeStruct(queries.shape, BF16), jax.ShapeDtypeStruct(pages, BF16))
        out_specs = (hbm, hbm)
    else:
        out_shape, out_specs = jax.ShapeDtypeStruct(kept, F32), hbm

    def kernel(*refs):
        attend_kernel(groups, first, final, *refs)

    return pl.pallas_call(
        kernel,
        in_specs=in_specs,
        out_specs=out_specs,
        out_shape=out_shape,
        scratch_shapes=scratch,
        name="attend_last" if final else "attend_part",
    )(*operands)


def shards(queries, keys, values, lengths, page_owner, page_slot):
    tok_rows = keys.shape[0]
    slots = tok_rows // PAGE * 2
    seq_count = lax.axis_size("seq")
    mine = lax.axis_index("seq").astype(jnp.int32).reshape(1)
    lens = lengths.reshape(1, -1)
    flat_q = queries.transpose(1, 0, 2)

    own, outgoing = pack_pages(keys, values, page_owner.T, page_slot.T, seq_count)
    b6 = shifted(own, 6)
    b3 = shifted(own, 3)
    b1 = shifted(own, 1)

    got = lax.all_to_all(
        outgoing.reshape(seq_count, CHUNKS, 2, HD), "seq", split_axis=0, concat_axis=0, tiled=True
    )

    b47 = shifted(jnp.concatenate([b3, b6]), 1)
    b2 = shifted(b1, 1)
    groups = [(0, 0, 0), (1, 0, 1), (2, 0, 3), (3, 0, 6)]
    state = attend(mine, lens, flat_q, [own, b1, b3, b6], groups, None)
    b58 = shifted(b47, 1)
    groups = [(0, 0, 2), (1, 0, 4), (1, 1, 7)]
    state = attend(mine, lens, flat_q, [b2, b47], groups, state)
    got = got.reshape(seq_count * CHUNKS * 2, HD)
    out, placed = attend(mine, lens, flat_q, [b58], [(0, 0, 5), (0, 1, 8)], state, got)
    attended = out.transpose(1, 0, 2)
    cache_pages = (
        placed.reshape(slots, 2, PAGE, HD).transpose(0, 2, 1, 3).reshape(slots, PAGE, 2 * HD)
    )
    return (attended, cache_pages)


def solution(mesh):
    placed = (
        P(("group", "seq"), None, "head"),
        P(("group", "seq"), "head"),
        P(("group", "seq"), "head"),
        P("group"),
        P(("group", "seq"), "head"),
        P(("group", "seq"), "head"),
    )
    return jax.shard_map(
        shards,
        mesh=mesh,
        in_specs=placed,
        out_specs=(P(("group", "seq"), None, "head"), P(("group", "seq", "head"), None, None)),
        check_vma=False,
    )
```

```python
import math

import jax
import jax.numpy as jnp
from jax import lax
from jax.experimental import pallas as pl
from jax.experimental.pallas import tpu as pltpu
from jax.sharding import PartitionSpec as P


QPER = 5
HD = 128
PAGE = 4
CHUNKS = PAGE + 1
NEG = -1e30
PAIR = 2
F32 = jnp.float32
BF16 = jnp.bfloat16

NT = (((1,), (1,)), ((), ()))
NN = (((1,), (0,)), ((), ()))
TN = (((0,), (0,)), ((), ()))


def dot(a, b, dims=NN):
    return lax.dot_general(a, b, dims, preferred_element_type=F32)


def shifted(x, by):
    count = lax.axis_size("seq")
    pairs = [(i, i + by) for i in range(count - by)]
    return lax.ppermute(x, "seq", pairs)


def near_core(x):
    return pltpu.with_memory_space_constraint(x, pltpu.VMEM)


def pack_kernel(keys_ref, vals_ref, owner_ref, slot_ref, own_ref, out_ref):
    for c in range(2):
        own_ref[c * HD : (c + 1) * HD] = keys_ref[:, c * HD : (c + 1) * HD]
        own_ref[(2 + c) * HD : (3 + c) * HD] = vals_ref[:, c * HD : (c + 1) * HD].T
    rows = keys_ref.shape[0]
    pages = rows // PAGE
    per = CHUNKS * 2
    total = out_ref.shape[0]
    page_i = lax.broadcasted_iota(jnp.int32, (pages, rows), 0)
    tok_i = lax.broadcasted_iota(jnp.int32, (pages, rows), 1)
    spread = (tok_i // PAGE == page_i).astype(BF16)
    owner = dot(owner_ref[...].astype(BF16), spread).astype(jnp.int32)
    slot = dot(slot_ref[...].astype(BF16), spread).astype(jnp.int32)
    within = lax.broadcasted_iota(jnp.int32, (1, rows), 1) % PAGE
    keyed, tagged, onehot = [], [], []
    lane_id = lax.broadcasted_iota(jnp.int32, (HD, rows), 0)
    for c in range(2):
        base = owner[c : c + 1] * per
        keyed += [base + within * 2, base + within * 2 + 1]
        tagged.append(jnp.where(within == 0, base + PAGE * 2, -1))
        onehot.append((slot[c : c + 1] == lane_id).astype(BF16))
    parts = []
    for c in range(2):
        parts += [keys_ref[:, c * HD : (c + 1) * HD], vals_ref[:, c * HD : (c + 1) * HD]]
    step = 2 * HD
    for begin in range(0, total, step):
        row = begin + lax.broadcasted_iota(jnp.int32, (step, rows), 0)
        acc = jnp.zeros((step, HD), F32)
        for key, part in zip(keyed, parts):
            acc += dot((row == key).astype(BF16), part)
        for key, hot in zip(tagged, onehot):
            acc += dot((row == key).astype(BF16), hot, NT)
        out_ref[begin : begin + step] = acc.astype(BF16)


def pack_pages(keys, values, owner, slot, seq_count):
    return pl.pallas_call(
        pack_kernel,
        out_shape=(
            pltpu.VMEM((4 * HD, keys.shape[0]), BF16),
            pltpu.VMEM((seq_count * CHUNKS * 2, HD), BF16),
        ),
        name="pack_pages",
    )(keys, values, owner, slot)


def place_kernel(got_ref, out_ref):
    total = got_ref.shape[0]
    per = CHUNKS * 2
    sources = total // per
    pages = PAGE * 2
    slots = out_ref.shape[0] // pages
    got = got_ref[...]
    row = lax.broadcasted_iota(jnp.int32, (1, total), 1)
    source, inside = row // per, row % per
    src = lax.broadcasted_iota(jnp.int32, (sources, 1), 0)
    hot = dot((row == src * per + pages).astype(BF16), got).astype(BF16)[:, :slots]
    chosen = dot(hot, (source == src).astype(BF16), TN).astype(BF16)
    dst = lax.broadcasted_iota(jnp.int32, (slots * pages, 1), 0)
    slot = lax.broadcasted_iota(jnp.int32, (1, slots), 1)
    wide = dot((dst // pages == slot).astype(BF16), chosen).astype(BF16)
    want = (dst % PAGE) * 2 + dst % pages // PAGE
    step = 2 * HD
    for begin in range(0, slots * pages, step):
        here = slice(begin, begin + step)
        placed = jnp.where(want[here] == inside, wide[here], jnp.zeros((), BF16))
        out_ref[here] = dot(placed, got).astype(BF16)


def place_pages(got, slots):
    return pl.pallas_call(
        place_kernel,
        out_shape=jax.ShapeDtypeStruct((slots * PAGE * 2, HD), BF16),
        name="place_pages",
    )(got)


def attend_kernel(groups, first, final, *refs):
    refs = list(refs)
    mine_ref, lens_ref, q_ref = refs[:3]
    arrays = 1 + max(g[0] for g in groups)
    kv = refs[3 : 3 + arrays]
    rest = refs[3 + arrays :]
    if not first:
        acc_in, stats_in = rest[:2]
        rest = rest[2:]
    if final:
        result_ref, sems, staged = rest
    else:
        acc_ref, stats_ref = rest
    layers, rows, width = q_ref.shape
    wide = QPER * HD
    units = layers * width // wide
    reqs = lens_ref.shape[1]

    def send(i):
        lanes = pl.ds(pl.multiple_of(i % (width // wide) * wide, HD), wide)
        return pltpu.make_async_copy(
            staged.at[i], result_ref.at[i // (width // wide), :, lanes], sems.at[i]
        )

    base = mine_ref[0] * rows
    lens = jnp.broadcast_to(lens_ref[...], (reqs, reqs)).astype(F32)
    r_i = lax.broadcasted_iota(jnp.int32, (reqs, reqs), 0)
    e_i = lax.broadcasted_iota(jnp.int32, (reqs, reqs), 1)
    starts = jnp.sum(jnp.where(e_i < r_i, lens, 0.0), axis=1, keepdims=True) - base.astype(F32)
    lane = lax.broadcasted_iota(jnp.int32, (1, rows), 1)
    known = jnp.where(starts <= lane.astype(F32), starts, -3e7)
    begin = jnp.max(known, axis=0, keepdims=True).astype(jnp.int32)
    earliest = jnp.min(begin)
    factor = math.log2(math.e) / math.sqrt(HD)

    def take(some, i):
        head = i % (width // wide)
        layer = i // (width // wide)
        if not first:
            old = stats_in[i, 0:1]
            old_total = stats_in[i, 8:9]
        if some:
            key_i = lax.broadcasted_iota(jnp.int32, (rows, rows), 0)
            qry_i = lax.broadcasted_iota(jnp.int32, (rows, rows), 1)
            keys, vals, masks = [], [], []
            for source, index, distance in some:
                at = pl.multiple_of((4 * index + head) * HD, HD)
                keys.append(kv[source][pl.ds(at, HD)])
                vals.append(kv[source][pl.ds(at + 2 * HD, HD)])
                inside = key_i >= begin + distance * rows
                masks.append(inside & (key_i <= qry_i) if distance == 0 else inside)
            v_all = jnp.concatenate(vals, axis=1)
            lanes = [pl.ds(pl.multiple_of((head * QPER + q) * HD, HD), HD) for q in range(QPER)]
            queries = jnp.concatenate([q_ref[layer, :, at] for at in lanes], axis=0)
            scores = dot(jnp.concatenate(keys, axis=0), queries, NT) * factor
            allowed = jnp.concatenate([jnp.concatenate(masks, axis=0)] * QPER, axis=1)
            scores = jnp.where(allowed, scores, NEG)
            top = jnp.max(scores, axis=0, keepdims=True)
            if not first:
                top = jnp.maximum(old, top)
            weights = jnp.exp2(scores - top)
            total = jnp.sum(weights, axis=0, keepdims=True)
            acc = dot(v_all, weights.astype(BF16))
            if not first:
                shrink = jnp.exp2(old - top)
                total += old_total * shrink
                acc += acc_in[i].astype(F32) * shrink
        if final:
            if not some:
                total, acc = old_total, acc_in[i].astype(F32)
            normed = (acc * (1.0 / total)).astype(BF16)
            for q in range(QPER):
                staged[i, :, q * HD : (q + 1) * HD] = normed[:, q * rows : (q + 1) * rows].T
        elif some:
            acc_ref[i] = acc.astype(BF16)
            stats_ref[i, :8] = jnp.broadcast_to(top, (8, wide))
            stats_ref[i, 8:] = jnp.broadcast_to(total, (8, wide))
        else:
            acc_ref[i] = acc_in[i]
            stats_ref[i] = stats_in[i]

    for used in range(1 if first else 0, len(groups) + 1):
        some = groups[:used]
        case = True
        if used and some[-1][2]:
            case = earliest < rows - some[-1][2] * rows
        if used < len(groups):
            case = jnp.logical_and(case, earliest >= rows - groups[used][2] * rows)

        @pl.when(case)
        def _(some=some):
            @pl.loop(0, units, step=PAIR)
            def _(i):
                for j in range(PAIR):
                    take(some, i + j)
                if final:
                    for j in range(PAIR):
                        send(i + j).start()

    if final:
        for i in range(units):
            send(i).wait()


def attend(mine, lengths, queries, arrays, groups, state, final):
    layers, rows, width = queries.shape
    units = layers * width // (QPER * HD)
    first = state is None
    in_specs = [
        pl.BlockSpec(memory_space=pltpu.SMEM),
        pl.BlockSpec(memory_space=pltpu.VMEM),
        pl.BlockSpec(memory_space=pltpu.VMEM),
    ]
    in_specs += [pl.BlockSpec(memory_space=pltpu.VMEM) for _ in arrays]
    kept = ((units, HD, QPER * rows), BF16), ((units, 16, QPER * rows), F32)
    operands = [mine, lengths, near_core(queries), *map(near_core, arrays)]
    if not first:
        in_specs += [pl.BlockSpec(memory_space=pltpu.VMEM)] * 2
        operands += map(near_core, state)
    if final:
        out_shape = jax.ShapeDtypeStruct(queries.shape, BF16)
        out_specs = pl.BlockSpec(memory_space=pl.ANY)
        scratch = [
            pltpu.SemaphoreType.DMA((units,)),
            pltpu.VMEM((units, rows, QPER * HD), BF16),
        ]
    else:
        out_shape = tuple(pltpu.VMEM(*k) for k in kept)
        out_specs = (pl.BlockSpec(memory_space=pltpu.VMEM),) * 2
        scratch = []
    aliases = {} if first or final else {len(operands) - 2: 0, len(operands) - 1: 1}

    def kernel(*refs):
        attend_kernel(groups, first, final, *refs)

    return pl.pallas_call(
        kernel,
        in_specs=in_specs,
        out_specs=out_specs,
        out_shape=out_shape,
        scratch_shapes=scratch,
        input_output_aliases=aliases,
        name="attend_last" if final else "attend_part",
    )(*operands)


def shards(queries, keys, values, lengths, page_owner, page_slot):
    tok_rows = keys.shape[0]
    slots = tok_rows // PAGE * 2
    seq_count = lax.axis_size("seq")
    mine = lax.axis_index("seq").astype(jnp.int32).reshape(1)
    lens = lengths.reshape(1, -1)
    flat_q = queries.transpose(1, 0, 2)

    own, outgoing = pack_pages(keys, values, page_owner.T, page_slot.T, seq_count)
    b6 = shifted(own, 6)
    b3 = shifted(own, 3)
    b1 = shifted(own, 1)

    got = lax.all_to_all(
        outgoing.reshape(seq_count, CHUNKS, 2, HD), "seq", split_axis=0, concat_axis=0, tiled=True
    )

    b47 = shifted(jnp.concatenate([b3, b6]), 1)
    b2 = shifted(b1, 1)
    groups = [(0, 0, 0), (1, 0, 1), (2, 0, 3), (3, 0, 6)]
    state = attend(mine, lens, flat_q, [own, b1, b3, b6], groups, None, False)
    b58 = shifted(b47, 1)
    groups = [(0, 0, 2), (1, 0, 4), (1, 1, 7)]
    state = attend(mine, lens, flat_q, [b2, b47], groups, state, False)
    out = attend(mine, lens, flat_q, [b58], [(0, 0, 5), (0, 1, 8)], state, True)
    attended = out.transpose(1, 0, 2)

    placed = place_pages(got.reshape(seq_count * CHUNKS * 2, HD), slots)
    cache_pages = (
        placed.reshape(slots, 2, PAGE, HD).transpose(0, 2, 1, 3).reshape(slots, PAGE, 2 * HD)
    )
    return (attended, cache_pages)


def solution(mesh):
    placed = (
        P(("group", "seq"), None, "head"),
        P(("group", "seq"), "head"),
        P(("group", "seq"), "head"),
        P("group"),
        P(("group", "seq"), "head"),
        P(("group", "seq"), "head"),
    )
    return jax.shard_map(
        shards,
        mesh=mesh,
        in_specs=placed,
        out_specs=(P(("group", "seq"), None, "head"), P(("group", "seq", "head"), None, None)),
        check_vma=False,
    )
```

```python
import math

import jax
import jax.numpy as jnp
from jax import lax
from jax.experimental import pallas as pl
from jax.experimental.pallas import tpu as pltpu
from jax.sharding import PartitionSpec as P


QPER = 5
HD = 128
PAGE = 4
CHUNKS = PAGE + 1
NEG = -1e30
PAIR = 2
F32 = jnp.float32
BF16 = jnp.bfloat16

NT = (((1,), (1,)), ((), ()))
NN = (((1,), (0,)), ((), ()))
TN = (((0,), (0,)), ((), ()))


def dot(a, b, dims=NN):
    return lax.dot_general(a, b, dims, preferred_element_type=F32)


def shifted(x, by):
    count = lax.axis_size("seq")
    pairs = [(i, i + by) for i in range(count - by)]
    return lax.ppermute(x, "seq", pairs)


def near_core(x):
    return pltpu.with_memory_space_constraint(x, pltpu.VMEM)


def pack_kernel(keys_ref, vals_ref, owner_ref, slot_ref, own_ref, out_ref):
    for c in range(2):
        own_ref[c] = keys_ref[:, c * HD : (c + 1) * HD]
        own_ref[2 + c] = vals_ref[:, c * HD : (c + 1) * HD].T
    rows = keys_ref.shape[0]
    pages = rows // PAGE
    per = CHUNKS * 2
    total = out_ref.shape[0]
    page_i = lax.broadcasted_iota(jnp.int32, (pages, rows), 0)
    tok_i = lax.broadcasted_iota(jnp.int32, (pages, rows), 1)
    spread = (tok_i // PAGE == page_i).astype(BF16)
    owner = dot(owner_ref[...].astype(BF16), spread).astype(jnp.int32)
    slot = dot(slot_ref[...].astype(BF16), spread).astype(jnp.int32)
    within = lax.broadcasted_iota(jnp.int32, (1, rows), 1) % PAGE
    keyed, tagged, onehot = [], [], []
    lane_id = lax.broadcasted_iota(jnp.int32, (HD, rows), 0)
    for c in range(2):
        base = owner[c : c + 1] * per
        keyed += [base + within * 2, base + within * 2 + 1]
        tagged.append(jnp.where(within == 0, base + PAGE * 2, -1))
        onehot.append((slot[c : c + 1] == lane_id).astype(BF16))
    parts = []
    for c in range(2):
        parts += [keys_ref[:, c * HD : (c + 1) * HD], vals_ref[:, c * HD : (c + 1) * HD]]
    step = 5 * HD
    for begin in range(0, total, step):
        row = begin + lax.broadcasted_iota(jnp.int32, (step, rows), 0)
        acc = jnp.zeros((step, HD), F32)
        for key, part in zip(keyed, parts):
            acc += dot((row == key).astype(BF16), part)
        for key, hot in zip(tagged, onehot):
            acc += dot((row == key).astype(BF16), hot, NT)
        out_ref[begin : begin + step] = acc.astype(BF16)


def pack_pages(keys, values, owner, slot, seq_count):
    return pl.pallas_call(
        pack_kernel,
        out_shape=(
            pltpu.VMEM((4, HD, keys.shape[0]), BF16),
            pltpu.VMEM((seq_count * CHUNKS * 2, HD), BF16),
        ),
        name="pack_pages",
    )(keys, values, owner, slot)


def place_kernel(got_ref, out_ref):
    total = got_ref.shape[0]
    per = CHUNKS * 2
    sources = total // per
    pages = PAGE * 2
    slots = out_ref.shape[0] // pages
    got = got_ref[...]
    row = lax.broadcasted_iota(jnp.int32, (1, total), 1)
    source, inside = row // per, row % per
    src = lax.broadcasted_iota(jnp.int32, (sources, 1), 0)
    hot = dot((row == src * per + pages).astype(BF16), got).astype(BF16)[:, :slots]
    chosen = dot(hot, (source == src).astype(BF16), TN).astype(BF16)
    dst = lax.broadcasted_iota(jnp.int32, (slots * pages, 1), 0)
    slot = lax.broadcasted_iota(jnp.int32, (1, slots), 1)
    wide = dot((dst // pages == slot).astype(BF16), chosen).astype(BF16)
    want = (dst % PAGE) * 2 + dst % pages // PAGE
    step = 2 * HD
    for begin in range(0, slots * pages, step):
        here = slice(begin, begin + step)
        placed = jnp.where(want[here] == inside, wide[here], jnp.zeros((), BF16))
        out_ref[here] = dot(placed, got).astype(BF16)


def place_pages(got, slots):
    return pl.pallas_call(
        place_kernel,
        out_shape=jax.ShapeDtypeStruct((slots * PAGE * 2, HD), BF16),
        name="place_pages",
    )(near_core(got))


def attend_kernel(groups, first, final, *refs):
    refs = list(refs)
    mine_ref, lens_ref, q_ref = refs[:3]
    arrays = 1 + max(g[0] for g in groups)
    kv = refs[3 : 3 + arrays]
    rest = refs[3 + arrays :]
    state_in = None if first else rest.pop(0)
    result_ref = rest.pop(0)
    work, sems = rest[:2]
    staged = rest[2] if final else None
    layers, rows, width = q_ref.shape
    wide = QPER * HD
    units = layers * width // wide
    reqs = lens_ref.shape[1]

    def fetch(i):
        return pltpu.make_async_copy(state_in.at[i], work.at[i], sems.at[0, i])

    def send(i):
        if not final:
            return pltpu.make_async_copy(work.at[i], result_ref.at[i], sems.at[1, i])
        lanes = pl.ds(pl.multiple_of(i % (width // wide) * wide, HD), wide)
        return pltpu.make_async_copy(
            staged.at[i], result_ref.at[i // (width // wide), :, lanes], sems.at[1, i]
        )

    if not first:
        for i in range(units):
            fetch(i).start()

    base = mine_ref[0] * rows
    lens = jnp.broadcast_to(lens_ref[...], (reqs, reqs)).astype(F32)
    r_i = lax.broadcasted_iota(jnp.int32, (reqs, reqs), 0)
    e_i = lax.broadcasted_iota(jnp.int32, (reqs, reqs), 1)
    starts = jnp.sum(jnp.where(e_i < r_i, lens, 0.0), axis=1, keepdims=True) - base.astype(F32)
    lane = lax.broadcasted_iota(jnp.int32, (1, rows), 1)
    known = jnp.where(starts <= lane.astype(F32), starts, -3e7)
    begin = jnp.max(known, axis=0, keepdims=True).astype(jnp.int32)
    earliest = jnp.min(begin)
    factor = math.log2(math.e) / math.sqrt(HD)

    def take(some, i):
        head = i % (width // wide)
        layer = i // (width // wide)
        if not first:
            old = work[i, HD : HD + 1]
            old_total = work[i, HD + 8 : HD + 9]
        if some:
            key_i = lax.broadcasted_iota(jnp.int32, (rows, rows), 0)
            qry_i = lax.broadcasted_iota(jnp.int32, (rows, rows), 1)
            keys, vals, masks = [], [], []
            for source, index, distance in some:
                ref = kv[source]
                keys.append(ref[head] if index is None else ref[index, head])
                vals.append(ref[2 + head] if index is None else ref[index, 2 + head])
                inside = key_i >= begin + distance * rows
                masks.append(inside & (key_i <= qry_i) if distance == 0 else inside)
            v_all = jnp.concatenate(vals, axis=1)
            lanes = [pl.ds(pl.multiple_of((head * QPER + q) * HD, HD), HD) for q in range(QPER)]
            queries = jnp.concatenate([q_ref[layer, :, at] for at in lanes], axis=0)
            scores = dot(jnp.concatenate(keys, axis=0), queries, NT) * factor
            allowed = jnp.concatenate([jnp.concatenate(masks, axis=0)] * QPER, axis=1)
            scores = jnp.where(allowed, scores, NEG)
            top = jnp.max(scores, axis=0, keepdims=True)
            if not first:
                top = jnp.maximum(old, top)
            weights = jnp.exp2(scores - top)
            total = jnp.sum(weights, axis=0, keepdims=True)
            acc = dot(v_all, weights.astype(BF16))
            if not first:
                shrink = jnp.exp2(old - top)
                total += old_total * shrink
                acc += work[i, :HD] * shrink
        if final:
            if not some:
                total, acc = old_total, work[i, :HD]
            normed = (acc * (1.0 / total)).astype(BF16)
            for q in range(QPER):
                staged[i, :, q * HD : (q + 1) * HD] = normed[:, q * rows : (q + 1) * rows].T
        elif some:
            work[i, :HD] = acc
            work[i, HD : HD + 8] = jnp.broadcast_to(top, (8, wide))
            work[i, HD + 8 :] = jnp.broadcast_to(total, (8, wide))

    for used in range(1 if first else 0, len(groups) + 1):
        some = groups[:used]
        case = True
        if used and some[-1][2]:
            case = earliest < rows - some[-1][2] * rows
        if used < len(groups):
            case = jnp.logical_and(case, earliest >= rows - groups[used][2] * rows)

        @pl.when(case)
        def _(some=some):
            @pl.loop(0, units, step=PAIR)
            def _(i):
                for j in range(PAIR):
                    if not first:
                        fetch(i + j).wait()
                for j in range(PAIR):
                    take(some, i + j)
                for j in range(PAIR):
                    send(i + j).start()

    for i in range(units):
        send(i).wait()


def attend(mine, lengths, queries, arrays, groups, state, final):
    layers, rows, width = queries.shape
    units = layers * width // (QPER * HD)
    first = state is None
    in_specs = [
        pl.BlockSpec(memory_space=pltpu.SMEM),
        pl.BlockSpec(memory_space=pltpu.VMEM),
        pl.BlockSpec(memory_space=pltpu.VMEM),
    ]
    in_specs += [pl.BlockSpec(memory_space=pltpu.VMEM) for _ in arrays]
    kept = (units, HD + 16, QPER * rows)
    operands = [mine, lengths, near_core(queries), *map(near_core, arrays)]
    if not first:
        in_specs.append(pl.BlockSpec(memory_space=pl.ANY))
        operands.append(state)
    scratch = [pltpu.VMEM(kept, F32), pltpu.SemaphoreType.DMA((2, units))]
    if final:
        scratch.append(pltpu.VMEM((units, rows, QPER * HD), BF16))
        out_shape = jax.ShapeDtypeStruct(queries.shape, BF16)
    else:
        out_shape = jax.ShapeDtypeStruct(kept, F32)

    def kernel(*refs):
        attend_kernel(groups, first, final, *refs)

    return pl.pallas_call(
        kernel,
        in_specs=in_specs,
        out_specs=pl.BlockSpec(memory_space=pl.ANY),
        out_shape=out_shape,
        scratch_shapes=scratch,
        name="attend_last" if final else "attend_part",
    )(*operands)


def shards(queries, keys, values, lengths, page_owner, page_slot):
    tok_rows = keys.shape[0]
    slots = tok_rows // PAGE * 2
    seq_count = lax.axis_size("seq")
    mine = lax.axis_index("seq").astype(jnp.int32).reshape(1)
    lens = lengths.reshape(1, -1)
    flat_q = queries.transpose(1, 0, 2)

    own, outgoing = pack_pages(keys, values, page_owner.T, page_slot.T, seq_count)
    b6 = shifted(own, 6)
    b3 = shifted(own, 3)
    b1 = shifted(own, 1)

    got = lax.all_to_all(
        outgoing.reshape(seq_count, CHUNKS, 2, HD), "seq", split_axis=0, concat_axis=0, tiled=True
    )

    b47 = shifted(jnp.stack([b3, b6]), 1)
    b2 = shifted(b1, 1)
    groups = [(0, None, 0), (1, None, 1), (2, None, 3), (3, None, 6)]
    state = attend(mine, lens, flat_q, [own, b1, b3, b6], groups, None, False)
    b58 = shifted(b47, 1)
    groups = [(0, None, 2), (1, 0, 4), (1, 1, 7)]
    state = attend(mine, lens, flat_q, [b2, b47], groups, state, False)
    out = attend(mine, lens, flat_q, [b58], [(0, 0, 5), (0, 1, 8)], state, True)
    attended = out.transpose(1, 0, 2)

    placed = place_pages(got.reshape(seq_count * CHUNKS * 2, HD), slots)
    cache_pages = (
        placed.reshape(slots, 2, PAGE, HD).transpose(0, 2, 1, 3).reshape(slots, PAGE, 2 * HD)
    )
    return (attended, cache_pages)


def solution(mesh):
    placed = (
        P(("group", "seq"), None, "head"),
        P(("group", "seq"), "head"),
        P(("group", "seq"), "head"),
        P("group"),
        P(("group", "seq"), "head"),
        P(("group", "seq"), "head"),
    )
    return jax.shard_map(
        shards,
        mesh=mesh,
        in_specs=placed,
        out_specs=(P(("group", "seq"), None, "head"), P(("group", "seq", "head"), None, None)),
        check_vma=False,
    )
```
